32 devices in a mesh: rows: 32 (over z, y, x, core).
Axes of the slice: x: 2, y: 2, z: 4, core: 2. Of those that a mesh axis runs over, the one named last changes fastest.
Arguments:
- tile_values: float32 [3584, 128, 128], P('rows'), as said below
- tile_row: int32 [3584], P('rows'), may hold values from 0 to 15, as said below
- tile_slot: int32 [3584], P('rows'), may hold values from 0 to 47, as said below
- tile_count: int32 [32], P('rows'), may hold values from 48 to 112, as said below
- requests: int32 [32, 32, 1], P('rows'), may hold values from 0 to 15
- right_side: float32 [512, 4, 128], P('rows')
Outputs:
- solution: float32 [512, 4, 128], P('rows')
- hessenberg: float32 [4, 4, 3], replicated
The draws below stay inside these ranges and needn't reach their ends.
Inputs may be any that keep to these rules, and one draw needn't show every extreme that they name: `tile_row`: tile t < 16 of every device lies in block row t; it is the diagonal tile of that row. `tile_slot`: slot s < 16 is the device's own block s; slot 16 + o + q is the q-th block requested from device o; tile t < 48 of every device uses slot t. `tile_count`: some device uses all 112 slots. requests[d, o, q] is a block index among device o's 16 block rows. `tile_values`: tile t < 16 of every device holds the diagonal block of its row.
All inputs are finite; a program needn't handle non-finite values.
Results may differ from the reference program's by a relative error of at most 0.0003.
Values sent between devices are 32-bit elements; how exact they have to be, the bound alone decides.
A program may use at most 64 MiB of HBM per device.

```python
import jax
import jax.numpy as jnp
from jax import lax

BS = 128
RB = 16
NRHS = 4
REQ = 1
EXTRA = 64
ITERS = 3
BLOCKS = 512
SLOTS = 48
TILES_DEV = 112
NTILES = 3584
N_ROWS = 32


def draw_tile_values(key, part):
    position = jnp.arange(NTILES, dtype=jnp.int32)
    diagonal_tile = position % TILES_DEV < RB
    spread = 0.7 / jnp.sqrt(jnp.float32(BS * TILES_DEV / RB))
    noise_key = jax.random.fold_in(key, 11)
    scale_key = jax.random.fold_in(key, 12)
    noise = jax.random.normal(noise_key, (NTILES, BS, BS), jnp.float32)
    scales = jax.random.uniform(scale_key, (NTILES, BS), jnp.float32, 1.0, 2.0)
    boosted = jnp.where(diagonal_tile[:, None], scales, 0.0)
    identity = jnp.eye(BS, dtype=jnp.float32)
    return noise * spread + boosted[:, :, None] * identity[None, :, :]


def draw_tile_row(key, part):
    position = jnp.arange(NTILES, dtype=jnp.int32) % TILES_DEV
    chosen = jax.random.randint(jax.random.fold_in(key, 21), (NTILES,), 0, RB, dtype=jnp.int32)
    return jnp.where(position < RB, position, chosen).astype(jnp.int32)


def draw_tile_slot(key, part):
    position = jnp.arange(NTILES, dtype=jnp.int32) % TILES_DEV
    chosen = jax.random.randint(jax.random.fold_in(key, 31), (NTILES,), 0, SLOTS, dtype=jnp.int32)
    return jnp.where(position < SLOTS, position, chosen).astype(jnp.int32)


def draw_tile_count(key, part):
    devices = NTILES // TILES_DEV
    level = jax.random.randint(jax.random.fold_in(key, 41), (devices,), 0, 65, dtype=jnp.int32)
    counts = SLOTS + EXTRA * level * level // 4096
    busiest = jax.random.randint(jax.random.fold_in(key, 42), (), 0, devices, dtype=jnp.int32)
    return jnp.where(jnp.arange(devices, dtype=jnp.int32) == busiest, TILES_DEV, counts).astype(jnp.int32)


def draw_right_side(key, part):
    devices = BLOCKS // RB
    owner_of = (jnp.arange(BLOCKS, dtype=jnp.int32) // RB).astype(jnp.float32)
    ramp = 1.0 + 2.0 * owner_of / max(devices - 1, 1)
    rough = jnp.exp(jax.random.uniform(jax.random.fold_in(key, 51), (BLOCKS, NRHS, 1), jnp.float32, -0.7, 0.7))
    values = jax.random.normal(jax.random.fold_in(key, 52), (BLOCKS, NRHS, BS), jnp.float32)
    return values * rough * ramp[:, None, None]


def set_ends(result, stream_key, low, high):
    place = [jax.random.randint(jax.random.fold_in(stream_key, axis), (), 0, length) for axis, length in enumerate(result.shape)]
    longest = result.shape.index(max(result.shape))
    neighbour = place[:longest] + [(place[longest] + 1) % result.shape[longest]] + place[longest + 1:]
    return result.at[tuple(place)].set(low).at[tuple(neighbour)].set(high)


def setup_inputs(seed: int = 0) -> dict:
    key_of = jax.random.split(jax.random.key(seed), 7)
    return {
        "tile_values": draw_tile_values(jax.random.fold_in(key_of[6], 71), 0),
        "tile_row": draw_tile_row(jax.random.fold_in(key_of[6], 71), 0),
        "tile_slot": draw_tile_slot(jax.random.fold_in(key_of[6], 71), 0),
        "tile_count": draw_tile_count(jax.random.fold_in(key_of[6], 71), 0),
        "requests": set_ends(jax.random.randint(key_of[4], (N_ROWS, N_ROWS, REQ), 0, RB), jax.random.fold_in(key_of[4], 1), 0, RB - 1).astype(jnp.int32),
        "right_side": draw_right_side(jax.random.fold_in(key_of[6], 71), 0),
    }


epsilon = 1e-06
highest = lax.Precision.HIGHEST

def least_squares(hessenberg, beta_norm):
    krylov = hessenberg.shape[2]
    triangle = hessenberg
    target = jnp.zeros((hessenberg.shape[0], krylov + 1), jnp.float32).at[:, 0].set(beta_norm)
    cosines = []
    sine_list = []
    for column in range(krylov):
        column_vals = triangle[:, :, column]
        for earlier in range(column):
            first_entry = column_vals[:, earlier]
            second = column_vals[:, earlier + 1]
            column_vals = column_vals.at[:, earlier].set(cosines[earlier] * first_entry + sine_list[earlier] * second)
            column_vals = column_vals.at[:, earlier + 1].set(cosines[earlier] * second - sine_list[earlier] * first_entry)
        first_entry = column_vals[:, column]
        second = column_vals[:, column + 1]
        radius = jnp.sqrt(first_entry * first_entry + second * second)
        cosine = first_entry / radius
        sine_term = second / radius
        cosines.append(cosine)
        sine_list.append(sine_term)
        column_vals = column_vals.at[:, column].set(radius).at[:, column + 1].set(0.0)
        triangle = triangle.at[:, :, column].set(column_vals)
        leading = target[:, column]
        target = target.at[:, column].set(cosine * leading).at[:, column + 1].set(-sine_term * leading)
    weights = jnp.zeros((hessenberg.shape[0], krylov), jnp.float32)
    for column in reversed(range(krylov)):
        partial_sum = target[:, column] - lax.optimization_barrier(jnp.sum(triangle[:, column, column + 1:krylov] * weights[:, column + 1:], axis=1))
        weights = weights.at[:, column].set(partial_sum / triangle[:, column, column])
    return weights

def reference(tile_values, tile_row, tile_slot, tile_count, requests, right_side):
    tile_total = tile_slot.shape[0]
    position = jnp.arange(tile_total, dtype=jnp.int32)
    device = (position // TILES_DEV).astype(jnp.int32)
    shifted = jnp.maximum(tile_slot - RB, 0)
    owner_index = (shifted // REQ).astype(jnp.int32)
    within = (shifted % REQ).astype(jnp.int32)
    remote = requests[device, owner_index, within]
    columns = jnp.where(tile_slot < RB, device * RB + tile_slot, owner_index * RB + remote).astype(jnp.int32)
    rows_global = (device * RB + tile_row).astype(jnp.int32)
    live_mask = (position % TILES_DEV < tile_count[device]).astype(jnp.float32)

    def apply_matrix(vector):
        picked = vector[columns]
        products = jnp.einsum('tij,tkj->tki', tile_values, picked, precision=highest)
        products = products * live_mask[:, None, None]
        return jax.ops.segment_sum(products, rows_global, num_segments=vector.shape[0])
    beta_norm = jnp.sqrt(lax.optimization_barrier(jnp.sum(right_side * right_side, axis=(0, 2))) + epsilon)
    basis_list = [right_side / beta_norm[None, :, None]]
    hessenberg = jnp.zeros((right_side.shape[1], ITERS + 1, ITERS), jnp.float32)
    for column in range(ITERS):
        candidate = apply_matrix(basis_list[column])
        for earlier in range(column + 1):
            projection = lax.optimization_barrier(jnp.sum(candidate * basis_list[earlier], axis=(0, 2)))
            hessenberg = hessenberg.at[:, earlier, column].set(projection)
            candidate = candidate - projection[None, :, None] * basis_list[earlier]
        length = jnp.sqrt(lax.optimization_barrier(jnp.sum(candidate * candidate, axis=(0, 2))) + epsilon)
        hessenberg = hessenberg.at[:, column + 1, column].set(length)
        if column + 1 < ITERS:
            basis_list.append(candidate / length[None, :, None])
    weights = least_squares(hessenberg, beta_norm)
    stacked = jnp.stack(basis_list)
    solution = jnp.einsum('kj,jrki->rki', weights, stacked, precision=highest)
    return (solution, hessenberg)
```

```python
import functools

import jax
import jax.numpy as jnp
from jax import lax
from jax.experimental import pallas as pl
from jax.experimental.pallas import tpu as pltpu
from jax.sharding import PartitionSpec as P

ITERS = 3
MESH = pl.DeviceIdType.MESH
epsilon = 1e-06
f32 = jnp.float32
bf16 = jnp.bfloat16


def split(x):
    high = x.astype(bf16).astype(f32)
    return high, x - high


def dot(a, b):
    return lax.dot_general(a, b, (((1,), (0,)), ((), ())), preferred_element_type=f32)


def dot_nt(a, b):
    return lax.dot_general(a, b, (((1,), (1,)), ((), ())), preferred_element_type=f32)


def twice(x):
    return jnp.concatenate([x, x], axis=0)


def kernel(
    n,
    chunk,
    unroll,
    tile_hbm,
    row_ref,
    count_ref,
    slot_ref,
    request_ref,
    right_ref,
    out_ref,
    hess_ref,
    tiles,
    parts,
    selector,
    spread,
    asked,
    outgoing,
    incoming,
    own,
    slots,
    table,
    products,
    tile_sem,
    ask_send,
    ask_recv,
    send_sem,
    recv_sem,
):
    me = lax.axis_index("rows")
    total, size, _ = tiles.shape
    blocks, systems, _ = right_ref.shape
    rows = 2 * systems
    chunks = total // chunk

    def tile_copy(index):
        where = pl.ds(index * chunk, chunk)
        return pltpu.make_async_copy(tile_hbm.at[where], tiles.at[where], tile_sem.at[index])

    for index in range(chunks):
        tile_copy(index).start()

    def peer_of(step):
        return lax.rem(me + step, n)

    def each_peer(body):
        def run(step, carry):
            body(step, peer_of(step))
            return carry

        lax.fori_loop(1, n, run, 0, unroll=min(unroll, n - 1))

    barrier = pltpu.get_barrier_semaphore()
    each_peer(
        lambda step, peer: pl.semaphore_signal(
            barrier, inc=1, device_id=(peer,), device_id_type=MESH
        )
    )

    lane = lax.broadcasted_iota(jnp.int32, (1, total), 1)
    live_row = jnp.where(lane < count_ref[0], row_ref[...], blocks)
    wide = total * rows
    from_tile = lax.broadcasted_iota(jnp.int32, (total, wide), 0)
    to_column = lax.broadcasted_iota(jnp.int32, (total, wide), 1)
    expand = jnp.where(to_column // rows == from_tile, 1.0, 0.0).astype(bf16)
    row_of = dot(jnp.broadcast_to(live_row.astype(f32), (8, total)).astype(bf16), expand)[0:1]
    for block in range(blocks):
        k_row = lax.broadcasted_iota(jnp.int32, (rows, wide), 0)
        q_col = lax.broadcasted_iota(jnp.int32, (rows, wide), 1)
        fits = (k_row % systems == q_col % systems) & (
            jnp.broadcast_to(row_of, (rows, wide)) == float(block)
        )
        spread[pl.ds(block * rows, rows), :] = jnp.where(fits, 1.0, 0.0)
    selector[...] = spread[...].astype(bf16)

    for block in range(blocks):
        own[0, block] = twice(right_ref[block])

    pl.semaphore_wait(barrier, n - 1)

    def ask_copy(step, peer):
        return pltpu.make_async_remote_copy(
            src_ref=request_ref,
            dst_ref=asked.at[me],
            send_sem=ask_send.at[step],
            recv_sem=ask_recv.at[me],
            device_id=(peer,),
            device_id_type=MESH,
        )

    def ask_arrival(peer):
        return pltpu.make_async_remote_copy(
            src_ref=request_ref,
            dst_ref=asked.at[peer],
            send_sem=ask_send.at[0],
            recv_sem=ask_recv.at[peer],
            device_id=(peer,),
            device_id_type=MESH,
        )

    each_peer(lambda step, peer: ask_copy(step, peer).start())

    def split_chunk(index, carry):
        tile_copy(index).wait()

        def split_tile(offset, carry):
            tile = index * chunk + offset
            high, low = split(tiles[tile])
            parts[tile, :, 0:size] = high.astype(bf16)
            parts[tile, :, size : 2 * size] = low.astype(bf16)
            return carry

        return lax.fori_loop(0, chunk, split_tile, carry, unroll=4)

    lax.fori_loop(0, chunks, split_chunk, 0)

    each_peer(lambda step, peer: ask_arrival(peer).wait_recv())
    each_peer(lambda step, peer: ask_copy(step, peer).wait_send())

    sub = lax.broadcasted_iota(jnp.int32, (rows, size), 0)
    lanes = lax.broadcasted_iota(jnp.int32, (rows, size), 1)
    system_of = sub % systems

    def message(parity, step, peer):
        return pltpu.make_async_remote_copy(
            src_ref=outgoing.at[parity, peer, pl.ds(0, systems + 1)],
            dst_ref=incoming.at[parity, me, pl.ds(0, systems + 1)],
            send_sem=send_sem.at[parity, peer],
            recv_sem=recv_sem.at[parity, me],
            device_id=(peer,),
            device_id_type=MESH,
        )

    def arrival(parity, peer):
        return pltpu.make_async_remote_copy(
            src_ref=outgoing.at[parity, peer, pl.ds(0, systems + 1)],
            dst_ref=incoming.at[parity, peer, pl.ds(0, systems + 1)],
            send_sem=send_sem.at[parity, peer],
            recv_sem=recv_sem.at[parity, peer],
            device_id=(peer,),
            device_id_type=MESH,
        )

    def exchange(parity, vector, sums):
        packed = jnp.zeros((rows, size), f32)
        for position, entry in enumerate(sums):
            packed = packed + jnp.where(lanes == rows * position + sub, entry, 0.0)
        packed = jnp.sum(packed[0:systems], axis=0, keepdims=True)
        incoming[parity, me, pl.ds(systems, 1), :] = packed

        def send(step, peer):
            outgoing[parity, peer, pl.ds(0, systems), :] = own[vector, asked[peer, 0, me]][0:systems]
            outgoing[parity, peer, pl.ds(systems, 1), :] = packed
            message(parity, step, peer).start()

        each_peer(send)

    def arrive(parity, count):
        each_peer(lambda step, peer: arrival(parity, peer).wait_recv())
        each_peer(lambda step, peer: message(parity, step, peer).wait_send())
        whole = jnp.sum(incoming[parity, :, systems, :], axis=0, keepdims=True)
        whole = jnp.broadcast_to(whole, (rows, size))
        return [
            jnp.broadcast_to(
                jnp.sum(
                    jnp.where(lanes == rows * position + system_of, whole, 0.0),
                    axis=1,
                    keepdims=True,
                ),
                (rows, size),
            )
            for position in range(count)
        ]

    def local_sum(x, y):
        return jnp.sum(jnp.sum(x * y, axis=0), axis=1, keepdims=True)

    def multiply():
        def step(group, carry):
            for offset in range(8):
                tile = group * 8 + offset
                x = table[slot_ref[tile]].astype(bf16)
                y = dot_nt(jnp.concatenate([x, x], axis=1), parts[tile])
                products[pl.ds(pl.multiple_of(tile * rows, rows), rows), :] = y
            return carry

        lax.fori_loop(0, total // 8, step, 0)
        high, low = split(products[...])
        result = dot(selector[...], high.astype(bf16)) + dot(selector[...], low.astype(bf16))
        return result.reshape(blocks, rows, size)

    def fill(index, scale, coefficients, parity):
        def place(slot, raw):
            for earlier, value in enumerate(coefficients):
                raw = raw - value * slots[earlier, slot]
            raw = raw * scale
            slots[index, slot] = raw
            high, low = split(raw)
            table[slot] = jnp.where(sub < systems, high, low)

        for block in range(blocks):
            place(block, own[index, block])

        def run(peer, carry):
            place(blocks + peer, twice(incoming[parity, peer, pl.ds(0, systems), :]))
            return carry

        lax.fori_loop(0, n, run, 0, unroll=min(8, n))

    def keep_own(parity, vector):
        incoming[parity, me, pl.ds(0, systems), :] = own[vector, request_ref[0, me]][0:systems]

    zero = jnp.zeros((rows, size), f32)
    right = own[0]
    exchange(0, 0, [local_sum(right, right)])
    keep_own(0, 0)
    (square,) = arrive(0, 1)
    beta = jnp.sqrt(square + epsilon)
    scale = 1.0 / beta
    gram = {(0, 0): square * scale * scale}
    coefficients = []
    triangle = []
    raw_columns = []
    rotations = []
    target = [beta]
    parity = 0
    for column in range(ITERS):
        fill(column, scale, coefficients, parity)
        candidate = multiply()
        parity = (column + 1) % 2
        sums = [local_sum(candidate, slots[i, 0:blocks]) for i in range(column + 1)]
        sums.append(local_sum(candidate, candidate))
        if column + 1 < ITERS:
            own[column + 1] = candidate
            exchange(parity, column + 1, sums)
            keep_own(parity, column + 1)
        else:
            own[ITERS] = candidate
            exchange(parity, column + 1, sums)
        if column >= 1:
            rotate(raw_columns[column - 1], rotations, triangle, target)
        summed = arrive(parity, column + 2)

        def inner(i, j):
            return gram[(min(i, j), max(i, j))]

        coefficients = []
        for i in range(column + 1):
            value = summed[i]
            for earlier in range(i):
                value = value - coefficients[earlier] * inner(earlier, i)
            coefficients.append(value)
        residual = summed[column + 1]
        for i in range(column + 1):
            residual = residual - 2.0 * coefficients[i] * summed[i]
        for i in range(column + 1):
            for j in range(column + 1):
                residual = residual + coefficients[i] * coefficients[j] * inner(i, j)
        residual = jnp.maximum(residual, 0.0)
        length = jnp.sqrt(residual + epsilon)
        scale = 1.0 / length
        if column + 1 < ITERS:
            for i in range(column + 1):
                value = summed[i]
                for earlier in range(column + 1):
                    value = value - coefficients[earlier] * inner(earlier, i)
                gram[(i, column + 1)] = value * scale
            gram[(column + 1, column + 1)] = residual * scale * scale
        raw_columns.append(coefficients + [length])
    rotate(raw_columns[ITERS - 1], rotations, triangle, target)
    weights = [None] * ITERS
    for column in reversed(range(ITERS)):
        value = target[column]
        for later in range(column + 1, ITERS):
            value = value - triangle[later][column] * weights[later]
        weights[column] = value / triangle[column][column]
    solved = weights[0] * slots[0, 0:blocks]
    for i in range(1, ITERS):
        solved = solved + weights[i] * slots[i, 0:blocks]
    for block in range(blocks):
        out_ref[block] = solved[block, 0:systems]
    for system in range(systems):
        picture = zero
        for column in range(ITERS):
            for i in range(column + 2):
                picture = jnp.where(
                    (sub == i) & (lanes == column),
                    jnp.broadcast_to(raw_columns[column][i][system : system + 1], (rows, size)),
                    picture,
                )
        hess_ref[system] = picture[0 : ITERS + 1, 0:ITERS]


def rotate(column, rotations, triangle, target):
    column = list(column)
    for i, (cosine, sine) in enumerate(rotations):
        first, second = column[i], column[i + 1]
        column[i] = cosine * first + sine * second
        column[i + 1] = cosine * second - sine * first
    last = len(column) - 2
    first, second = column[last], column[last + 1]
    radius = jnp.sqrt(first * first + second * second)
    cosine, sine = first / radius, second / radius
    rotations.append((cosine, sine))
    column[last] = radius
    triangle.append(column[: last + 1])
    leading = target[last]
    target[last] = cosine * leading
    target.append(-sine * leading)


def on_device(tile_values, tile_row, tile_slot, tile_count, requests, right_side):
    n = lax.axis_size("rows")
    total, size, _ = tile_values.shape
    blocks, systems, _ = right_side.shape
    rows = 2 * systems
    chunk = 16 if total % 16 == 0 else 1
    smem = pl.BlockSpec(memory_space=pltpu.SMEM)
    vmem = pl.BlockSpec(memory_space=pltpu.VMEM)
    dma = pltpu.SemaphoreType.DMA
    return pl.pallas_call(
        functools.partial(kernel, n, chunk, 8),
        out_shape=(
            jax.ShapeDtypeStruct((blocks, systems, size), f32),
            jax.ShapeDtypeStruct((systems, ITERS + 1, ITERS), f32),
        ),
        in_specs=[pl.BlockSpec(memory_space=pl.ANY), vmem, smem, smem, smem, vmem],
        out_specs=(vmem, vmem),
        scratch_shapes=[
            pltpu.VMEM((total, size, size), f32),
            pltpu.VMEM((total, size, 2 * size), bf16),
            pltpu.VMEM((blocks * rows, total * rows), bf16),
            pltpu.VMEM((blocks * rows, total * rows), f32),
            pltpu.SMEM((n, 1, n), jnp.int32),
            pltpu.VMEM((2, n, 8, size), f32),
            pltpu.VMEM((2, n, 8, size), f32),
            pltpu.VMEM((ITERS + 1, blocks, rows, size), f32),
            pltpu.VMEM((ITERS, blocks + n, rows, size), f32),
            pltpu.VMEM((blocks + n, rows, size), f32),
            pltpu.VMEM((total * rows, size), f32),
            dma((total // chunk,)),
            dma((n,)),
            dma((n,)),
            dma((2, n)),
            dma((2, n)),
        ],
        compiler_params=pltpu.CompilerParams(
            collective_id=0, has_side_effects=True, vmem_limit_bytes=60 * 1024 * 1024
        ),
        name="cycle",
    )(
        tile_values,
        tile_row.reshape(1, total),
        tile_count,
        tile_slot,
        requests.reshape(1, n),
        right_side,
    )


def solution(mesh):
    return jax.shard_map(
        on_device,
        mesh=mesh,
        in_specs=(
            P("rows", None, None),
            P("rows"),
            P("rows"),
            P("rows"),
            P("rows", None, None),
            P("rows", None, None),
        ),
        out_specs=(P("rows", None, None), P()),
        check_vma=False,
    )
```

```python
import functools

import jax
import jax.numpy as jnp
from jax import lax
from jax.experimental import pallas as pl
from jax.experimental.pallas import tpu as pltpu
from jax.sharding import PartitionSpec as P

ITERS = 3
MESH = pl.DeviceIdType.MESH
epsilon = 1e-06
f32 = jnp.float32
bf16 = jnp.bfloat16


def split(x):
    high = x.astype(bf16).astype(f32)
    return high, x - high


def dot(a, b):
    return lax.dot_general(a, b, (((1,), (0,)), ((), ())), preferred_element_type=f32)


def twice(x):
    return jnp.concatenate([x, x], axis=0)


def kernel(
    n,
    chunk,
    unroll,
    tile_hbm,
    row_ref,
    count_ref,
    slot_ref,
    request_ref,
    right_ref,
    out_ref,
    hess_ref,
    tiles,
    parts,
    selector,
    spread,
    asked,
    outgoing,
    incoming,
    own,
    slots,
    table,
    products,
    tile_sem,
    ask_send,
    ask_recv,
    send_sem,
    recv_sem,
):
    me = lax.axis_index("rows")
    total, size, _ = tiles.shape
    blocks, systems, _ = right_ref.shape
    rows = 2 * systems
    chunks = total // chunk
    batch = max(b for b in range(1, 57) if total % b == 0)

    def tile_copy(index):
        where = pl.ds(index * chunk, chunk)
        return pltpu.make_async_copy(tile_hbm.at[where], tiles.at[where], tile_sem.at[index])

    for index in range(chunks):
        tile_copy(index).start()

    def peer_of(step):
        return lax.rem(me + step, n)

    def each_peer(body):
        def run(step, carry):
            body(step, peer_of(step))
            return carry

        lax.fori_loop(1, n, run, 0, unroll=min(unroll, n - 1))

    barrier = pltpu.get_barrier_semaphore()
    each_peer(
        lambda step, peer: pl.semaphore_signal(
            barrier, inc=1, device_id=(peer,), device_id_type=MESH
        )
    )

    lane = lax.broadcasted_iota(jnp.int32, (1, total), 1)
    live_row = jnp.where(lane < count_ref[...], row_ref[...], blocks)
    wide = total * rows
    from_tile = lax.broadcasted_iota(jnp.int32, (total, wide), 0)
    to_column = lax.broadcasted_iota(jnp.int32, (total, wide), 1)
    expand = jnp.where(to_column // rows == from_tile, 1.0, 0.0).astype(bf16)
    row_of = dot(jnp.broadcast_to(live_row.astype(f32), (8, total)).astype(bf16), expand)[0:1]
    for block in range(blocks):
        k_row = lax.broadcasted_iota(jnp.int32, (rows, wide), 0)
        q_col = lax.broadcasted_iota(jnp.int32, (rows, wide), 1)
        fits = (k_row % systems == q_col % systems) & (
            jnp.broadcast_to(row_of, (rows, wide)) == float(block)
        )
        spread[pl.ds(block * rows, rows), :] = jnp.where(fits, 1.0, 0.0)
    selector[...] = spread[...].astype(bf16)

    for block in range(blocks):
        own[0, block] = twice(right_ref[block])

    pl.semaphore_wait(barrier, n - 1)

    def ask_copy(step, peer):
        return pltpu.make_async_remote_copy(
            src_ref=request_ref,
            dst_ref=asked.at[me],
            send_sem=ask_send.at[step],
            recv_sem=ask_recv.at[me],
            device_id=(peer,),
            device_id_type=MESH,
        )

    def ask_arrival(peer):
        return pltpu.make_async_remote_copy(
            src_ref=request_ref,
            dst_ref=asked.at[peer],
            send_sem=ask_send.at[0],
            recv_sem=ask_recv.at[peer],
            device_id=(peer,),
            device_id_type=MESH,
        )

    each_peer(lambda step, peer: ask_copy(step, peer).start())

    def split_chunk(index, carry):
        tile_copy(index).wait()

        def split_tile(offset, carry):
            tile = index * chunk + offset
            high, low = split(tiles[tile].T)
            parts[tile, 0:size, :] = high.astype(bf16)
            parts[tile, size : 2 * size, :] = low.astype(bf16)
            return carry

        return lax.fori_loop(0, chunk, split_tile, carry, unroll=4)

    lax.fori_loop(0, chunks, split_chunk, 0)

    each_peer(lambda step, peer: ask_arrival(peer).wait_recv())
    each_peer(lambda step, peer: ask_copy(step, peer).wait_send())

    sub = lax.broadcasted_iota(jnp.int32, (rows, size), 0)
    lanes = lax.broadcasted_iota(jnp.int32, (rows, size), 1)
    system_of = sub % systems

    def message(parity, step, peer):
        return pltpu.make_async_remote_copy(
            src_ref=outgoing.at[parity, peer, pl.ds(0, systems + 1)],
            dst_ref=incoming.at[parity, me, pl.ds(0, systems + 1)],
            send_sem=send_sem.at[parity, peer],
            recv_sem=recv_sem.at[parity, me],
            device_id=(peer,),
            device_id_type=MESH,
        )

    def arrival(parity, peer):
        return pltpu.make_async_remote_copy(
            src_ref=outgoing.at[parity, peer, pl.ds(0, systems + 1)],
            dst_ref=incoming.at[parity, peer, pl.ds(0, systems + 1)],
            send_sem=send_sem.at[parity, peer],
            recv_sem=recv_sem.at[parity, peer],
            device_id=(peer,),
            device_id_type=MESH,
        )

    def exchange(parity, vector, sums):
        packed = jnp.zeros((rows, size), f32)
        for position, entry in enumerate(sums):
            packed = packed + jnp.where(lanes == rows * position + sub, entry, 0.0)
        packed = jnp.sum(packed[0:systems], axis=0, keepdims=True)
        incoming[parity, me, pl.ds(systems, 1), :] = packed

        def send(step, peer):
            outgoing[parity, peer, pl.ds(0, systems), :] = own[vector, asked[peer, 0, me]][0:systems]
            outgoing[parity, peer, pl.ds(systems, 1), :] = packed
            message(parity, step, peer).start()

        each_peer(send)

    def arrive(parity, count):
        each_peer(lambda step, peer: arrival(parity, peer).wait_recv())
        each_peer(lambda step, peer: message(parity, step, peer).wait_send())
        whole = jnp.sum(incoming[parity, :, systems, :], axis=0, keepdims=True)
        whole = jnp.broadcast_to(whole, (rows, size))
        return [
            jnp.broadcast_to(
                jnp.sum(
                    jnp.where(lanes == rows * position + system_of, whole, 0.0),
                    axis=1,
                    keepdims=True,
                ),
                (rows, size),
            )
            for position in range(count)
        ]

    def local_sum(x, y):
        return jnp.sum(jnp.sum(x * y, axis=0), axis=1, keepdims=True)

    def multiply():
        def step(group, carry):
            for offset in range(batch):
                tile = group * batch + offset
                x = table[slot_ref[tile]].astype(bf16)
                y = dot(jnp.concatenate([x, x], axis=1), parts[tile])
                products[pl.ds(pl.multiple_of(tile * rows, rows), rows), :] = y
            return carry

        lax.fori_loop(0, total // batch, step, 0)
        high, low = split(products[...])
        result = dot(selector[...], high.astype(bf16)) + dot(selector[...], low.astype(bf16))
        return result.reshape(blocks, rows, size)

    def fill(index, scale, coefficients, parity):
        def place(slot, raw):
            for earlier, value in enumerate(coefficients):
                raw = raw - value * slots[earlier, slot]
            raw = raw * scale
            slots[index, slot] = raw
            high, low = split(raw)
            table[slot] = jnp.where(sub < systems, high, low)

        for block in range(blocks):
            place(block, own[index, block])

        def run(peer, carry):
            place(blocks + peer, twice(incoming[parity, peer, pl.ds(0, systems), :]))
            return carry

        lax.fori_loop(0, n, run, 0, unroll=min(8, n))

    def keep_own(parity, vector):
        incoming[parity, me, pl.ds(0, systems), :] = own[vector, request_ref[0, me]][0:systems]

    zero = jnp.zeros((rows, size), f32)
    right = own[0]
    exchange(0, 0, [local_sum(right, right)])
    keep_own(0, 0)
    (square,) = arrive(0, 1)
    beta = jnp.sqrt(square + epsilon)
    scale = 1.0 / beta
    gram = {(0, 0): square * scale * scale}
    coefficients = []
    triangle = []
    raw_columns = []
    rotations = []
    target = [beta]
    parity = 0
    for column in range(ITERS):
        fill(column, scale, coefficients, parity)
        candidate = multiply()
        parity = (column + 1) % 2
        sums = [local_sum(candidate, slots[i, 0:blocks]) for i in range(column + 1)]
        sums.append(local_sum(candidate, candidate))
        if column + 1 < ITERS:
            own[column + 1] = candidate
            exchange(parity, column + 1, sums)
            keep_own(parity, column + 1)
        else:
            own[ITERS] = candidate
            exchange(parity, column + 1, sums)
        if column >= 1:
            rotate(raw_columns[column - 1], rotations, triangle, target)
        summed = arrive(parity, column + 2)

        def inner(i, j):
            return gram[(min(i, j), max(i, j))]

        coefficients = []
        for i in range(column + 1):
            value = summed[i]
            for earlier in range(i):
                value = value - coefficients[earlier] * inner(earlier, i)
            coefficients.append(value)
        residual = summed[column + 1]
        for i in range(column + 1):
            residual = residual - 2.0 * coefficients[i] * summed[i]
        for i in range(column + 1):
            for j in range(column + 1):
                residual = residual + coefficients[i] * coefficients[j] * inner(i, j)
        residual = jnp.maximum(residual, 0.0)
        length = jnp.sqrt(residual + epsilon)
        scale = 1.0 / length
        if column + 1 < ITERS:
            for i in range(column + 1):
                value = summed[i]
                for earlier in range(column + 1):
                    value = value - coefficients[earlier] * inner(earlier, i)
                gram[(i, column + 1)] = value * scale
            gram[(column + 1, column + 1)] = residual * scale * scale
        raw_columns.append(coefficients + [length])
    rotate(raw_columns[ITERS - 1], rotations, triangle, target)
    weights = [None] * ITERS
    for column in reversed(range(ITERS)):
        value = target[column]
        for later in range(column + 1, ITERS):
            value = value - triangle[later][column] * weights[later]
        weights[column] = value / triangle[column][column]
    solved = weights[0] * slots[0, 0:blocks]
    for i in range(1, ITERS):
        solved = solved + weights[i] * slots[i, 0:blocks]
    for block in range(blocks):
        out_ref[block] = solved[block, 0:systems]
    for system in range(systems):
        picture = zero
        for column in range(ITERS):
            for i in range(column + 2):
                picture = jnp.where(
                    (sub == i) & (lanes == column),
                    jnp.broadcast_to(raw_columns[column][i][system : system + 1], (rows, size)),
                    picture,
                )
        hess_ref[system] = picture[0 : ITERS + 1, 0:ITERS]


def rotate(column, rotations, triangle, target):
    column = list(column)
    for i, (cosine, sine) in enumerate(rotations):
        first, second = column[i], column[i + 1]
        column[i] = cosine * first + sine * second
        column[i + 1] = cosine * second - sine * first
    last = len(column) - 2
    first, second = column[last], column[last + 1]
    radius = jnp.sqrt(first * first + second * second)
    cosine, sine = first / radius, second / radius
    rotations.append((cosine, sine))
    column[last] = radius
    triangle.append(column[: last + 1])
    leading = target[last]
    target[last] = cosine * leading
    target.append(-sine * leading)


def on_device(tile_values, tile_row, tile_slot, tile_count, requests, right_side):
    n = lax.axis_size("rows")
    total, size, _ = tile_values.shape
    blocks, systems, _ = right_side.shape
    rows = 2 * systems
    chunk = 16 if total % 16 == 0 else 1
    smem = pl.BlockSpec(memory_space=pltpu.SMEM)
    vmem = pl.BlockSpec(memory_space=pltpu.VMEM)
    dma = pltpu.SemaphoreType.DMA
    return pl.pallas_call(
        functools.partial(kernel, n, chunk, 8),
        out_shape=(
            jax.ShapeDtypeStruct((blocks, systems, size), f32),
            jax.ShapeDtypeStruct((systems, ITERS + 1, ITERS), f32),
        ),
        in_specs=[pl.BlockSpec(memory_space=pl.ANY), vmem, vmem, smem, smem, vmem],
        out_specs=(vmem, vmem),
        scratch_shapes=[
            pltpu.VMEM((total, size, size), f32),
            pltpu.VMEM((total, 2 * size, size), bf16),
            pltpu.VMEM((blocks * rows, total * rows), bf16),
            pltpu.VMEM((blocks * rows, total * rows), f32),
            pltpu.SMEM((n, 1, n), jnp.int32),
            pltpu.VMEM((2, n, 8, size), f32),
            pltpu.VMEM((2, n, 8, size), f32),
            pltpu.VMEM((ITERS + 1, blocks, rows, size), f32),
            pltpu.VMEM((ITERS, blocks + n, rows, size), f32),
            pltpu.VMEM((blocks + n, rows, size), f32),
            pltpu.VMEM((total * rows, size), f32),
            dma((total // chunk,)),
            dma((n,)),
            dma((n,)),
            dma((2, n)),
            dma((2, n)),
        ],
        compiler_params=pltpu.CompilerParams(
            collective_id=0, has_side_effects=True, vmem_limit_bytes=60 * 1024 * 1024
        ),
        name="cycle",
    )(
        tile_values,
        tile_row.reshape(1, total),
        tile_count.reshape(1, 1),
        tile_slot,
        requests.reshape(1, n),
        right_side,
    )


def solution(mesh):
    return jax.shard_map(
        on_device,
        mesh=mesh,
        in_specs=(
            P("rows", None, None),
            P("rows"),
            P("rows"),
            P("rows"),
            P("rows", None, None),
            P("rows", None, None),
        ),
        out_specs=(P("rows", None, None), P()),
        check_vma=False,
    )
```

```python
import functools

import jax
import jax.numpy as jnp
from jax import lax
from jax.experimental import pallas as pl
from jax.experimental.pallas import tpu as pltpu
from jax.sharding import PartitionSpec as P

ITERS = 3
MESH = pl.DeviceIdType.MESH
epsilon = 1e-06
f32 = jnp.float32
bf16 = jnp.bfloat16


def split(x):
    high = x.astype(bf16).astype(f32)
    return high, x - high


def dot(a, b):
    return lax.dot_general(a, b, (((1,), (0,)), ((), ())), preferred_element_type=f32)


def twice(x):
    return jnp.concatenate([x, x], axis=0)


def kernel(
    n,
    chunk,
    unroll,
    tile_hbm,
    row_ref,
    count_ref,
    slot_ref,
    request_ref,
    right_ref,
    out_ref,
    hess_ref,
    tiles,
    parts,
    selector,
    spread,
    asked,
    outgoing,
    incoming,
    own,
    slots,
    table,
    products,
    tile_sem,
    ask_send,
    ask_recv,
    send_sem,
    recv_sem,
):
    me = lax.axis_index("rows")
    total, size, _ = tiles.shape
    blocks, systems, _ = right_ref.shape
    rows = 2 * systems
    chunks = total // chunk
    batch = max(b for b in range(1, 57) if total % b == 0)

    def tile_copy(index):
        where = pl.ds(index * chunk, chunk)
        return pltpu.make_async_copy(tile_hbm.at[where], tiles.at[where], tile_sem.at[index])

    for index in range(chunks):
        tile_copy(index).start()

    def peer_of(step):
        return lax.rem(me + step, n)

    def each_peer(body):
        def run(step, carry):
            body(step, peer_of(step))
            return carry

        lax.fori_loop(1, n, run, 0, unroll=min(unroll, n - 1))

    barrier = pltpu.get_barrier_semaphore()
    each_peer(
        lambda step, peer: pl.semaphore_signal(
            barrier, inc=1, device_id=(peer,), device_id_type=MESH
        )
    )

    lane = lax.broadcasted_iota(jnp.int32, (1, total), 1)
    live_row = jnp.where(lane < count_ref[...], row_ref[...], blocks)
    wide = total * rows
    from_tile = lax.broadcasted_iota(jnp.int32, (total, wide), 0)
    to_column = lax.broadcasted_iota(jnp.int32, (total, wide), 1)
    expand = jnp.where(to_column // rows == from_tile, 1.0, 0.0).astype(bf16)
    row_of = dot(jnp.broadcast_to(live_row.astype(f32), (8, total)).astype(bf16), expand)[0:1]
    for block in range(blocks):
        k_row = lax.broadcasted_iota(jnp.int32, (rows, wide), 0)
        q_col = lax.broadcasted_iota(jnp.int32, (rows, wide), 1)
        fits = (k_row % systems == q_col % systems) & (
            jnp.broadcast_to(row_of, (rows, wide)) == float(block)
        )
        spread[pl.ds(block * rows, rows), :] = jnp.where(fits, 1.0, 0.0)
    selector[...] = spread[...].astype(bf16)

    for block in range(blocks):
        own[0, block] = twice(right_ref[block])

    pl.semaphore_wait(barrier, n - 1)

    def ask_copy(step, peer):
        return pltpu.make_async_remote_copy(
            src_ref=request_ref,
            dst_ref=asked.at[me],
            send_sem=ask_send.at[step],
            recv_sem=ask_recv.at[me],
            device_id=(peer,),
            device_id_type=MESH,
        )

    def ask_arrival(peer):
        return pltpu.make_async_remote_copy(
            src_ref=request_ref,
            dst_ref=asked.at[peer],
            send_sem=ask_send.at[0],
            recv_sem=ask_recv.at[peer],
            device_id=(peer,),
            device_id_type=MESH,
        )

    each_peer(lambda step, peer: ask_copy(step, peer).start())

    def split_chunk(index, carry):
        tile_copy(index).wait()

        def split_tile(offset, carry):
            tile = index * chunk + offset
            high, low = split(tiles[tile].T)
            parts[tile, 0:size, :] = high.astype(bf16)
            parts[tile, size : 2 * size, :] = low.astype(bf16)
            return carry

        return lax.fori_loop(0, chunk, split_tile, carry, unroll=4)

    lax.fori_loop(0, chunks, split_chunk, 0)

    each_peer(lambda step, peer: ask_arrival(peer).wait_recv())
    each_peer(lambda step, peer: ask_copy(step, peer).wait_send())

    sub = lax.broadcasted_iota(jnp.int32, (rows, size), 0)
    lanes = lax.broadcasted_iota(jnp.int32, (rows, size), 1)
    system_of = sub % systems

    def message(parity, step, peer):
        return pltpu.make_async_remote_copy(
            src_ref=outgoing.at[parity, peer, pl.ds(0, systems + 1)],
            dst_ref=incoming.at[parity, me, pl.ds(0, systems + 1)],
            send_sem=send_sem.at[parity, peer],
            recv_sem=recv_sem.at[parity, me],
            device_id=(peer,),
            device_id_type=MESH,
        )

    def arrival(parity, peer):
        return pltpu.make_async_remote_copy(
            src_ref=outgoing.at[parity, peer, pl.ds(0, systems + 1)],
            dst_ref=incoming.at[parity, peer, pl.ds(0, systems + 1)],
            send_sem=send_sem.at[parity, peer],
            recv_sem=recv_sem.at[parity, peer],
            device_id=(peer,),
            device_id_type=MESH,
        )

    def exchange(parity, vector, sums):
        packed = jnp.zeros((rows, size), f32)
        for position, entry in enumerate(sums):
            packed = packed + jnp.where(lanes == rows * position + sub, entry, 0.0)
        packed = jnp.sum(packed[0:systems], axis=0, keepdims=True)
        incoming[parity, me, pl.ds(systems, 1), :] = packed

        def send(step, peer):
            outgoing[parity, peer, pl.ds(0, systems), :] = own[vector, asked[peer, 0, me]][0:systems]
            outgoing[parity, peer, pl.ds(systems, 1), :] = packed
            message(parity, step, peer).start()

        each_peer(send)

    def arrive(parity, count):
        each_peer(lambda step, peer: arrival(parity, peer).wait_recv())
        each_peer(lambda step, peer: message(parity, step, peer).wait_send())
        whole = jnp.sum(incoming[parity, :, systems, :], axis=0, keepdims=True)
        whole = jnp.broadcast_to(whole, (rows, size))
        return [
            jnp.broadcast_to(
                jnp.sum(
                    jnp.where(lanes == rows * position + system_of, whole, 0.0),
                    axis=1,
                    keepdims=True,
                ),
                (rows, size),
            )
            for position in range(count)
        ]

    def local_sum(x, y):
        return jnp.sum(jnp.sum(x * y, axis=0), axis=1, keepdims=True)

    def multiply():
        def step(group, carry):
            for offset in range(batch):
                tile = group * batch + offset
                x = table[slot_ref[tile]].astype(bf16)
                y = dot(jnp.concatenate([x, x], axis=1), parts[tile])
                products[pl.ds(pl.multiple_of(tile * rows, rows), rows), :] = y
            return carry

        lax.fori_loop(0, total // batch, step, 0)
        high, low = split(products[...])
        result = dot(selector[...], high.astype(bf16)) + dot(selector[...], low.astype(bf16))
        return result.reshape(blocks, rows, size)

    def fill(index, scale, coefficients, parity):
        def place(slot, raw):
            for earlier, value in enumerate(coefficients):
                raw = raw - value * slots[earlier, slot]
            raw = raw * scale
            slots[index, slot] = raw
            high, low = split(raw)
            table[slot] = jnp.where(sub < systems, high, low)

        for block in range(blocks):
            place(block, own[index, block])

        def run(peer, carry):
            place(blocks + peer, twice(incoming[parity, peer, pl.ds(0, systems), :]))
            return carry

        lax.fori_loop(0, n, run, 0, unroll=min(8, n))

    def keep_own(parity, vector):
        incoming[parity, me, pl.ds(0, systems), :] = own[vector, request_ref[0, me]][0:systems]

    zero = jnp.zeros((rows, size), f32)
    right = own[0]
    exchange(0, 0, [local_sum(right, right)])
    keep_own(0, 0)
    (square,) = arrive(0, 1)
    beta = jnp.sqrt(square + epsilon)
    scale = 1.0 / beta
    gram = {(0, 0): square * scale * scale}
    coefficients = []
    triangle = []
    raw_columns = []
    rotations = []
    target = [beta]
    parity = 0
    for column in range(ITERS):
        fill(column, scale, coefficients, parity)
        candidate = multiply()
        parity = (column + 1) % 2
        sums = [local_sum(candidate, slots[i, 0:blocks]) for i in range(column + 1)]
        sums.append(local_sum(candidate, candidate))
        if column + 1 < ITERS:
            own[column + 1] = candidate
            exchange(parity, column + 1, sums)
            keep_own(parity, column + 1)
        else:
            own[ITERS] = candidate
            exchange(parity, column + 1, sums)
        if column >= 1:
            rotate(raw_columns[column - 1], rotations, triangle, target)
        summed = arrive(parity, column + 2)

        def inner(i, j):
            return gram[(min(i, j), max(i, j))]

        coefficients = []
        for i in range(column + 1):
            value = summed[i]
            for earlier in range(i):
                value = value - coefficients[earlier] * inner(earlier, i)
            coefficients.append(value)
        residual = summed[column + 1]
        for i in range(column + 1):
            residual = residual - 2.0 * coefficients[i] * summed[i]
        for i in range(column + 1):
            for j in range(column + 1):
                residual = residual + coefficients[i] * coefficients[j] * inner(i, j)
        residual = jnp.maximum(residual, 0.0)
        length = jnp.sqrt(residual + epsilon)
        scale = 1.0 / length
        if column + 1 < ITERS:
            for i in range(column + 1):
                value = summed[i]
                for earlier in range(column + 1):
                    value = value - coefficients[earlier] * inner(earlier, i)
                gram[(i, column + 1)] = value * scale
            gram[(column + 1, column + 1)] = residual * scale * scale
        raw_columns.append(coefficients + [length])
    rotate(raw_columns[ITERS - 1], rotations, triangle, target)
    weights = [None] * ITERS
    for column in reversed(range(ITERS)):
        value = target[column]
        for later in range(column + 1, ITERS):
            value = value - triangle[later][column] * weights[later]
        weights[column] = value / triangle[column][column]
    solved = weights[0] * slots[0, 0:blocks]
    for i in range(1, ITERS):
        solved = solved + weights[i] * slots[i, 0:blocks]
    for block in range(blocks):
        out_ref[block] = solved[block, 0:systems]
    for column in range(ITERS):
        picture = zero
        for i in range(column + 2):
            picture = jnp.where(lanes == i, raw_columns[column][i], picture)
        hess_ref[column] = picture[0:systems, 0 : ITERS + 1]


def rotate(column, rotations, triangle, target):
    column = list(column)
    for i, (cosine, sine) in enumerate(rotations):
        first, second = column[i], column[i + 1]
        column[i] = cosine * first + sine * second
        column[i + 1] = cosine * second - sine * first
    last = len(column) - 2
    first, second = column[last], column[last + 1]
    radius = jnp.sqrt(first * first + second * second)
    cosine, sine = first / radius, second / radius
    rotations.append((cosine, sine))
    column[last] = radius
    triangle.append(column[: last + 1])
    leading = target[last]
    target[last] = cosine * leading
    target.append(-sine * leading)


def hand_on(solved_ref, picture_ref, out_ref, hess_ref):
    out_ref[...] = solved_ref[...]
    hess_ref[...] = picture_ref[...]


def on_device(tile_values, tile_row, tile_slot, tile_count, requests, right_side):
    n = lax.axis_size("rows")
    total, size, _ = tile_values.shape
    blocks, systems, _ = right_side.shape
    rows = 2 * systems
    chunk = 16 if total % 16 == 0 else 1
    smem = pl.BlockSpec(memory_space=pltpu.SMEM)
    vmem = pl.BlockSpec(memory_space=pltpu.VMEM)
    dma = pltpu.SemaphoreType.DMA
    solved, picture = pl.pallas_call(
        functools.partial(kernel, n, chunk, 8),
        out_shape=(
            jax.ShapeDtypeStruct((blocks, systems, size), f32),
            jax.ShapeDtypeStruct((ITERS, systems, ITERS + 1), f32),
        ),
        in_specs=[pl.BlockSpec(memory_space=pl.ANY), vmem, vmem, smem, smem, vmem],
        out_specs=(vmem, vmem),
        scratch_shapes=[
            pltpu.VMEM((total, size, size), f32),
            pltpu.VMEM((total, 2 * size, size), bf16),
            pltpu.VMEM((blocks * rows, total * rows), bf16),
            pltpu.VMEM((blocks * rows, total * rows), f32),
            pltpu.SMEM((n, 1, n), jnp.int32),
            pltpu.VMEM((2, n, 8, size), f32),
            pltpu.VMEM((2, n, 8, size), f32),
            pltpu.VMEM((ITERS + 1, blocks, rows, size), f32),
            pltpu.VMEM((ITERS, blocks + n, rows, size), f32),
            pltpu.VMEM((blocks + n, rows, size), f32),
            pltpu.VMEM((total * rows, size), f32),
            dma((total // chunk,)),
            dma((n,)),
            dma((n,)),
            dma((2, n)),
            dma((2, n)),
        ],
        compiler_params=pltpu.CompilerParams(
            collective_id=0, has_side_effects=True, vmem_limit_bytes=60 * 1024 * 1024
        ),
        name="cycle",
    )(
        tile_values,
        tile_row.reshape(1, total),
        tile_count.reshape(1, 1),
        tile_slot,
        requests.reshape(1, n),
        right_side,
    )
    solved, picture = pl.pallas_call(
        hand_on,
        out_shape=(
            jax.ShapeDtypeStruct(solved.shape, f32),
            jax.ShapeDtypeStruct(picture.shape, f32),
        ),
        in_specs=[vmem, vmem],
        out_specs=(vmem, vmem),
        name="hand_on",
    )(solved, picture)
    return solved, jnp.transpose(picture, (1, 2, 0))


def solution(mesh):
    return jax.shard_map(
        on_device,
        mesh=mesh,
        in_specs=(
            P("rows", None, None),
            P("rows"),
            P("rows"),
            P("rows"),
            P("rows", None, None),
            P("rows", None, None),
        ),
        out_specs=(P("rows", None, None), P()),
        check_vma=False,
    )
```
